32 devices in a mesh: cp: 4 (over z), tp: 8 (over y, x, core).
Axes of the slice: x: 2, y: 2, z: 4, core: 2. Of those that a mesh axis runs over, the one named last changes fastest.
Arguments:
- checkpoint: bfloat16 [2048, 8192], P('cp', 'tp'), may hold values from -6 to 6
- norm_gain: float32 [8192], replicated, may hold values from 0.1 to 1.9
- query_weight: bfloat16 [8192, 8192], P(None, 'tp'), may hold values from -4 to 4
- key_weight: bfloat16 [8192, 1024], P(None, 'tp'), may hold values from -1 to 1
- value_weight: bfloat16 [8192, 1024], P(None, 'tp'), may hold values from -0.0625 to 0.0625
- output_weight: bfloat16 [8192, 8192], P('tp'), may hold values from -0.09375 to 0.09375
- block_order: int32 [8], replicated, may hold values from 0 to 7, each once
Outputs:
- projected: bfloat16 [2048, 8192], P('cp', 'tp')
- log_normalizer: float32 [64, 2048], P('tp', 'cp')
The draws below stay inside these ranges and needn't reach their ends.
Inputs may be any that keep to these rules, and one draw needn't show every extreme that they name: `block_order`: each of 0 to 7 once.
All inputs are finite; a program needn't handle non-finite values.
Results may differ from the reference program's by a relative error of at most 0.019.
Values may be sent and summed in bfloat16 or wider, within the bound.
A program may use at most 128 MiB of HBM per device.

```python
import math
import jax
import jax.numpy as jnp
from jax import lax

D = 8192
HEADS = 64
KV_HEADS = 8
HEAD_DIM = 128
SEQ = 2048
BLOCK = 256
N_CP = 4
N_TP = 8


def joint_query_key(key):
    shared_keys = jax.random.normal(jax.random.fold_in(key, 17), (D, KV_HEADS * HEAD_DIM), jnp.float32) / math.sqrt(D)
    shared_keys = jnp.clip(shared_keys, -1.0, 1.0)
    queries = jax.random.normal(jax.random.fold_in(key, 29), (D, HEADS * HEAD_DIM), jnp.float32) * (2.5 / math.sqrt(D))
    queries = jnp.clip(queries, -4.0, 4.0)
    return (queries, shared_keys)


def draw_query_weight(key, part):
    return joint_query_key(key)[0].astype(jnp.bfloat16)


def draw_key_weight(key, part):
    return joint_query_key(key)[1].astype(jnp.bfloat16)


def raised(values, stream_key, source, target, parts, factor):
    def block_of(axis_at):
        return (jnp.arange(values.shape[axis_at]) // (values.shape[axis_at] // parts)).reshape((-1,) + (1,) * (values.ndim - 1 - axis_at))

    first = jax.random.permutation(stream_key, parts)[block_of(target)]
    second = (block_of(target) + parts // 2) % parts
    return jnp.where((block_of(source) == first) | (block_of(source) == second), factor * values, values)


def steps_of(rng, dims, cuts, smallest, largest):
    def one(dim, blocks):
        steps = jax.random.uniform(jax.random.fold_in(jax.random.fold_in(rng, 6), dim), (blocks,), jnp.float32, smallest / len(cuts), largest / len(cuts))
        return jnp.repeat(jnp.exp(steps), dims[dim] // blocks).reshape((-1,) + (1,) * (len(dims) - dim - 1))

    gain = one(*cuts[0])
    for cut in cuts[1:]:
        gain = gain * one(*cut)
    return gain


def scatter_about(own_key, dims, spread, limit, shards=(), held_as=jnp.bfloat16):
    result = spread * jax.random.normal(own_key, dims, jnp.float32)
    if shards:
        result = result * steps_of(own_key, dims, shards, -0.22, 0.18)
    return jnp.clip(result, -limit, limit).astype(held_as)


def heavy_noise(own_key, shape, spread, limit, cuts, heavy, kind=jnp.bfloat16):
    entries = spread * jax.random.normal(own_key, shape, jnp.float32)
    if cuts:
        entries = entries * steps_of(own_key, shape, cuts, -0.22, 0.18)
    return jnp.clip(raised(entries, jax.random.fold_in(own_key, 3), *heavy), -limit, limit).astype(kind)


def setup_inputs(seed: int = 0) -> dict:
    streams_of = jax.random.split(jax.random.key(seed), 8)
    checkpoint = scatter_about(streams_of[0], (SEQ, D), 1.0, 6.0, ((0, 4), (1, 8)))
    norm_gain = jnp.clip(1.0 + 0.18 * jax.random.normal(streams_of[1], (D,), jnp.float32), 0.1, 1.9)
    query_weight = draw_query_weight(jax.random.fold_in(streams_of[7], 71), 0)
    key_weight = draw_key_weight(jax.random.fold_in(streams_of[7], 71), 0)
    value_weight = scatter_about(streams_of[4], (D, KV_HEADS * HEAD_DIM), D ** -0.5, 0.0625, ((1, 8),))
    output_weight = heavy_noise(streams_of[5], (HEADS * HEAD_DIM, D), (HEADS * HEAD_DIM) ** -0.5, 0.09375, ((0, 8),), (0, 1, 8, 2.0))
    block_order = jax.random.permutation(streams_of[6], 2 * N_CP).astype(jnp.int32)
    return {"checkpoint": checkpoint, "norm_gain": norm_gain, "query_weight": query_weight, "key_weight": key_weight, "value_weight": value_weight, "output_weight": output_weight, "block_order": block_order}


rope_base = 500000.0
norm_epsilon = 1e-05

def turn_pairs(matrix, positions, first_pair):
    pair_count = matrix.shape[-1] // 2
    pair_index = (first_pair + jnp.arange(pair_count, dtype=jnp.int32)).astype(jnp.float32)
    inverse_rates = rope_base ** (-2.0 * pair_index / HEAD_DIM)
    angles = positions.astype(jnp.float32)[:, None] * inverse_rates[None, :]
    cosine = jnp.cos(angles)[:, None, :]
    sine_part = jnp.sin(angles)[:, None, :]
    paired = matrix.reshape(matrix.shape[0], matrix.shape[1], pair_count, 2)
    former = paired[..., 0]
    latter = paired[..., 1]
    turned = jnp.stack([former * cosine - latter * sine_part, former * sine_part + latter * cosine], axis=-1)
    return turned.reshape(matrix.shape)

def reference(checkpoint, norm_gain, query_weight, key_weight, value_weight, output_weight, block_order):
    seq_rows = jnp.arange(SEQ, dtype=jnp.int32)
    positions = (block_order[seq_rows // BLOCK] * BLOCK + seq_rows % BLOCK).astype(jnp.int32)
    widened = checkpoint.astype(jnp.float32)
    mean_square = lax.optimization_barrier(jnp.mean(widened * widened, axis=-1, keepdims=True))
    normed = (widened * lax.rsqrt(mean_square + norm_epsilon) * norm_gain).astype(jnp.bfloat16)
    query_features = jnp.dot(normed, query_weight, preferred_element_type=jnp.float32)
    key_features = jnp.dot(normed, key_weight, preferred_element_type=jnp.float32)
    value_features = jnp.dot(normed, value_weight, preferred_element_type=jnp.float32)
    queries = turn_pairs(query_features.reshape(SEQ, HEADS, HEAD_DIM), positions, 0).astype(jnp.bfloat16)
    keys = turn_pairs(key_features.reshape(SEQ, KV_HEADS, HEAD_DIM), positions, 0).astype(jnp.bfloat16)
    values = value_features.astype(jnp.bfloat16).reshape(SEQ, KV_HEADS, HEAD_DIM)
    by_head_queries = jnp.transpose(queries, (1, 0, 2))
    key_heads = jnp.transpose(keys, (1, 0, 2))
    value_heads = jnp.transpose(values, (1, 0, 2))
    group_size = HEADS // KV_HEADS
    allowed = positions[None, :] <= positions[:, None]
    score_scale = 1.0 / math.sqrt(HEAD_DIM)

    def one_head(head_index):
        query_block = lax.dynamic_index_in_dim(by_head_queries, head_index, 0, keepdims=False)
        key_block = lax.dynamic_index_in_dim(key_heads, head_index // group_size, 0, keepdims=False)
        value_block = lax.dynamic_index_in_dim(value_heads, head_index // group_size, 0, keepdims=False)
        scores = jnp.dot(query_block, key_block.T, preferred_element_type=jnp.float32) * score_scale
        scores = jnp.where(allowed, scores, -jnp.inf)
        row_top = lax.optimization_barrier(jnp.max(scores, axis=-1, keepdims=True))
        normalizer = row_top + jnp.log(lax.optimization_barrier(jnp.sum(jnp.exp(scores - row_top), axis=-1, keepdims=True)))
        weights = jnp.exp(scores - normalizer).astype(jnp.bfloat16)
        attended_head = jnp.dot(weights, value_block, preferred_element_type=jnp.float32).astype(jnp.bfloat16)
        return (attended_head, normalizer[:, 0])
    attended, log_normalizer = lax.map(one_head, jnp.arange(HEADS, dtype=jnp.int32))
    attended_flat = jnp.transpose(attended, (1, 0, 2)).reshape(SEQ, HEADS * HEAD_DIM)
    group_rows = HEADS * HEAD_DIM // N_TP
    attended_groups = jnp.transpose(attended_flat.reshape(SEQ, N_TP, group_rows), (1, 0, 2))
    weight_groups = output_weight.reshape(N_TP, group_rows, D)

    def add_group(running_total, pieces):
        group_term = jnp.dot(pieces[0], pieces[1], preferred_element_type=jnp.float32).astype(jnp.bfloat16)
        group_term = lax.optimization_barrier(group_term)
        return (running_total + group_term.astype(jnp.float32), None)
    running_total, unused = lax.scan(add_group, jnp.zeros((SEQ, D), jnp.float32), (attended_groups, weight_groups))
    return (running_total.astype(jnp.bfloat16), log_normalizer)
```

```python
import functools
import math

import jax
import jax.numpy as jnp
from jax import lax
from jax.experimental import pallas as pl
from jax.experimental.pallas import tpu as pltpu
from jax.sharding import PartitionSpec as P

HEAD_DIM = 128
KV_HEADS = 8
MESH = pl.DeviceIdType.MESH
VMEM_BYTES = 62 * 1024 * 1024

rope_base = 500000.0
norm_epsilon = 1e-05
masked_score = -1e30
LOG2E = 1.4426950408889634


def partner_2(block, axis, stride):
    count = lax.axis_size(axis)
    route = []
    for low in range(count):
        high = low | 1 << stride
        if high != low and high < count:
            route += [(low, high), (high, low)]
    return lax.ppermute(block, axis, route)


def turn_pairs(matrix, positions, first_pair):
    pair_count = matrix.shape[-1] // 2
    pair_index = (first_pair + jnp.arange(pair_count, dtype=jnp.int32)).astype(jnp.float32)
    inverse_rates = rope_base ** (-2.0 * pair_index / HEAD_DIM)
    angles = positions.astype(jnp.float32)[:, None] * inverse_rates[None, :]
    cosine = jnp.cos(angles)[:, None, :]
    sine_part = jnp.sin(angles)[:, None, :]
    paired = matrix.reshape(matrix.shape[0], matrix.shape[1], pair_count, 2)
    former = paired[..., 0]
    latter = paired[..., 1]
    turned = jnp.stack(
        [former * cosine - latter * sine_part, former * sine_part + latter * cosine], axis=-1
    )
    return turned.reshape(matrix.shape)


def project_any(checkpoint, norm_gain, query_weight, key_weight, value_weight, positions):
    rows = checkpoint.shape[0]
    heads = query_weight.shape[1] // HEAD_DIM
    key_columns = key_weight.shape[1]
    gathered = lax.all_gather(checkpoint, "tp", axis=1, tiled=True)
    widened = gathered.astype(jnp.float32)
    mean_square = jnp.mean(widened * widened, axis=-1, keepdims=True)
    normed = (widened * lax.rsqrt(mean_square + norm_epsilon) * norm_gain).astype(jnp.bfloat16)
    query_features = jnp.dot(normed, query_weight, preferred_element_type=jnp.float32)
    key_features = jnp.dot(normed, key_weight, preferred_element_type=jnp.float32)
    value_features = jnp.dot(normed, value_weight, preferred_element_type=jnp.float32)
    turned = turn_pairs(query_features.reshape(rows, heads, HEAD_DIM), positions, 0)
    queries = (turned * (LOG2E / math.sqrt(HEAD_DIM))).astype(jnp.bfloat16)
    sharing = lax.axis_size("tp") // KV_HEADS
    part_of_head = lax.axis_index("tp") % sharing
    key_part = turn_pairs(
        key_features.reshape(rows, 1, key_columns), positions, part_of_head * (key_columns // 2)
    )
    key_part = key_part.astype(jnp.bfloat16).reshape(rows, key_columns)
    own_pair = jnp.stack([key_part, value_features.astype(jnp.bfloat16)])
    key_value = own_pair
    if sharing == 2:
        partner = partner_2(own_pair, "tp", 0)
        lower_first = jnp.concatenate([own_pair, partner], axis=-1)
        upper_first = jnp.concatenate([partner, own_pair], axis=-1)
        key_value = jnp.where(part_of_head == 0, lower_first, upper_first)
    return (
        queries.reshape(rows, heads * HEAD_DIM),
        jnp.concatenate([key_value[0], key_value[1]], axis=-1),
    )


def flipped(me, offset):
    result = me
    for bit in (1, 2, 4):
        if offset & bit:
            result = result + bit - 2 * bit * lax.rem(lax.div(me, bit), 2)
    return result


def greet(axis, others):
    barrier = pltpu.get_barrier_semaphore()
    for other in others:
        pl.semaphore_signal(barrier, inc=1, device_id={axis: other}, device_id_type=MESH)
    pl.semaphore_wait(barrier, len(others))


def sender(axis, send_sems, recv_sems):
    used = []

    def make(source, target, other):
        index = len(used)
        copy = pltpu.make_async_remote_copy(
            src_ref=source,
            dst_ref=target,
            send_sem=send_sems.at[index],
            recv_sem=recv_sems.at[index],
            device_id={axis: other},
            device_id_type=MESH,
        )
        used.append(copy)
        return copy

    return make, used


def project_kernel(
    x_hbm, gain_ref, wq_hbm, wk_hbm, wv_hbm, cos_ref, sin_ref,
    q_ref, kv_ref,
    held, weights, gains, acc, scaled, squares, x_sem, w_sems, send_sems, recv_sems,
):
    me = lax.axis_index("tp")
    rows, depth = x_hbm.shape
    half = rows // 2
    q_cols = wq_hbm.shape[1]
    k_cols = wk_hbm.shape[1]
    sib, nx, ny = flipped(me, 1), flipped(me, 2), flipped(me, 4)
    x_copy = pltpu.make_async_copy(x_hbm, held.at[0], x_sem)
    x_copy.start()
    w_copies = []
    for e in range(8):
        chunk = pl.ds(pl.multiple_of(flipped(me, e) * depth, depth), depth)
        parts = (
            (wq_hbm, 0, q_cols),
            (wk_hbm, q_cols, k_cols),
            (wv_hbm, q_cols + k_cols, k_cols),
        )
        w_copies.append(
            [
                pltpu.make_async_copy(
                    w.at[chunk, :], weights.at[e, :, pl.ds(at, size)], w_sems.at[e, i]
                )
                for i, (w, at, size) in enumerate(parts)
            ]
        )
    for copies in w_copies:
        for copy in copies:
            copy.start()
    greet("tp", (sib, nx, ny))
    x_copy.wait()
    make, used = sender("tp", send_sems, recv_sems)

    def part(slot, h):
        return held.at[slot, pl.ds(h * half, half), :]

    dx = [make(part(0, h), part(2, h), nx) for h in range(2)]
    dy = [make(part(0, h), part(4, h), ny) for h in range(2)]
    d1 = make(held.at[0], held.at[1], sib)
    forward_y = make(part(2, 0), part(6, 0), ny)
    forward_x = make(part(4, 1), part(6, 1), nx)
    d3 = [make(part(2, h), part(3, h), sib) for h in range(2)]
    d5 = [make(part(4, h), part(5, h), sib) for h in range(2)]
    d7 = [make(part(6, h), part(7, h), sib) for h in range(2)]
    dx[0].start()
    dy[1].start()
    dx[1].start()
    dy[0].start()
    d1.start()

    squares[...] = jnp.zeros_like(squares)
    acc[...] = jnp.zeros_like(acc)
    for e in range(8):
        gains[e] = gain_ref[pl.ds(flipped(me, e), 1), :]

    def process(e):
        for copy in w_copies[e]:
            copy.wait()

        @pl.loop(0, rows // 64)
        def _(i):
            at = pl.ds(pl.multiple_of(i * 64, 64), 64)
            wide = held[e, at, :].astype(jnp.float32)
            squares[at, :] += jnp.sum(wide * wide, axis=1, keepdims=True)
            scaled[at, :] = (wide * gains[e]).astype(jnp.bfloat16)

        @pl.loop(0, (q_cols + 2 * k_cols) // 256)
        def _(t):
            at = pl.ds(pl.multiple_of(t * 256, 256), 256)
            acc[:, at] += jnp.dot(
                scaled[...], weights[e, :, at], preferred_element_type=jnp.float32
            )

    process(0)
    d1.wait_recv()
    process(1)
    dx[0].wait_recv()
    forward_y.start()
    d3[0].start()
    dy[1].wait_recv()
    forward_x.start()
    d5[1].start()
    dx[1].wait_recv()
    d3[1].start()
    dy[0].wait_recv()
    d5[0].start()
    process(2)
    process(4)
    d3[0].wait_recv()
    d3[1].wait_recv()
    process(3)
    d5[0].wait_recv()
    d5[1].wait_recv()
    process(5)
    forward_y.wait_recv()
    d7[0].start()
    forward_x.wait_recv()
    d7[1].start()
    process(6)
    d7[0].wait_recv()
    d7[1].wait_recv()
    process(7)

    score_scale = LOG2E / math.sqrt(HEAD_DIM)
    features = depth * 8

    @pl.loop(0, rows // 64)
    def _(i):
        at = pl.ds(pl.multiple_of(i * 64, 64), 64)
        rate = lax.rsqrt(squares[at, :] * (1.0 / features) + norm_epsilon)
        cosine = cos_ref[at, :]
        sine = sin_ref[at, :]
        even = lax.rem(lax.broadcasted_iota(jnp.int32, (64, HEAD_DIM), 1), 2) == 0

        def turned(block):
            later = pltpu.roll(block, HEAD_DIM - 1, 1)
            former = pltpu.roll(block, 1, 1)
            return block * cosine + jnp.where(even, later, former) * sine

        for h in range(q_cols // HEAD_DIM):
            cols = pl.ds(h * HEAD_DIM, HEAD_DIM)
            q_ref[at, cols] = turned(acc[at, cols] * (rate * score_scale)).astype(jnp.bfloat16)
        keys = acc[at, pl.ds(q_cols, k_cols)] * rate
        kv_ref[at, pl.ds(0, k_cols)] = turned(keys).astype(jnp.bfloat16)
        values = acc[at, pl.ds(q_cols + k_cols, k_cols)] * rate
        kv_ref[at, pl.ds(k_cols, k_cols)] = values.astype(jnp.bfloat16)

    for copy in used:
        copy.wait_send()


def attend_kernel(
    n_cp, order_ref, q_ref, kv_hbm, out_ref, norm_ref,
    ring, extended, bias, top, weighted, norms, kv_sem, send_sems, recv_sems,
):
    me = lax.axis_index("cp")
    rows = q_ref.shape[0]
    block = rows // 2
    heads = q_ref.shape[1] // HEAD_DIM
    right, left = lax.rem(me + 1, n_cp), lax.rem(me + n_cp - 1, n_cp)
    own_copy = pltpu.make_async_copy(kv_hbm, ring.at[0], kv_sem)
    own_copy.start()
    greet("cp", (right, left))
    own_copy.wait()

    def hop(step, h):
        at = pl.ds(h * block, block)
        return pltpu.make_async_remote_copy(
            src_ref=ring.at[step, at, :],
            dst_ref=ring.at[step + 1, at, :],
            send_sem=send_sems.at[step, h],
            recv_sem=recv_sems.at[step, h],
            device_id={"cp": right},
            device_id_type=MESH,
        )

    hop(0, 0).start()
    hop(0, 1).start()
    extended[:, HEAD_DIM:] = jnp.ones((rows, HEAD_DIM), jnp.bfloat16)
    top[...] = jnp.full(top.shape, masked_score, jnp.float32)
    weighted[...] = jnp.zeros_like(weighted)

    def visit(step, carried):
        for h in range(2):

            @pl.when(step > 0)
            def _():
                hop(step - 1, h).wait_recv()

            @pl.when(jnp.logical_and(step > 0, step < n_cp - 1))
            def _():
                hop(step, h).start()

        owner = lax.rem(me - step + n_cp, n_cp)
        extended[:, :HEAD_DIM] = ring[step, :, HEAD_DIM:]
        base = lax.broadcasted_iota(jnp.int32, (block, block), 0) - lax.broadcasted_iota(
            jnp.int32, (block, block), 1
        )
        for i in range(2):
            for j in range(2):
                ahead = (order_ref[2 * me + i] - order_ref[2 * owner + j]) * block
                bias[i * block : (i + 1) * block, j * block : (j + 1) * block] = jnp.where(
                    base + ahead >= 0, 0.0, masked_score
                )

        def one_head(h, inner):
            cols = pl.ds(pl.multiple_of(h * HEAD_DIM, HEAD_DIM), HEAD_DIM)
            keys = ring[step, :, :HEAD_DIM]
            for i in range(2):
                at = pl.ds(i * block, block)
                scores = lax.dot_general(
                    q_ref[at, cols], keys, (((1,), (1,)), ((), ())),
                    preferred_element_type=jnp.float32,
                )
                scores = scores + bias[at, :]
                old_top = top[h, at, :]
                new_top = jnp.maximum(old_top, jnp.max(scores, axis=1, keepdims=True))
                weights = jnp.exp2(scores - new_top).astype(jnp.bfloat16)
                shrink = jnp.exp2(old_top - new_top)
                top[h, at, :] = new_top
                weighted[h, at, :] = weighted[h, at, :] * shrink + jnp.dot(
                    weights, extended[...], preferred_element_type=jnp.float32
                )
            return inner

        lax.fori_loop(0, heads, one_head, 0)
        return carried

    lax.fori_loop(0, n_cp, visit, 0)
    lane = lax.broadcasted_iota(jnp.int32, (rows, HEAD_DIM), 1)
    norms[...] = jnp.zeros_like(norms)
    for h in range(heads):
        totals = weighted[h, :, HEAD_DIM:]
        out_ref[:, h * HEAD_DIM : (h + 1) * HEAD_DIM] = (
            weighted[h, :, :HEAD_DIM] / totals
        ).astype(jnp.bfloat16)
        norm = (top[h] + jnp.log2(totals)) * (1.0 / LOG2E)
        norms[...] = jnp.where(lane == h, norm, norms[...])
    norm_ref[...] = jnp.transpose(norms[...])[:heads, :]

    for step in range(n_cp - 1):
        for h in range(2):
            hop(step, h).wait_send()


def output_kernel(
    a_ref, w_hbm, out_ref,
    weights, terms, sums, from_sib, from_six, from_x, from_y, w_sems, send_sems, recv_sems,
):
    me = lax.axis_index("tp")
    rows, depth = a_ref.shape
    cols = out_ref.shape[1]
    half = cols // 2
    sib, nx, ny = flipped(me, 1), flipped(me, 2), flipped(me, 4)
    order = [
        (7, 0), (6, 0), (7, 1), (6, 1), (3, 0), (2, 0), (5, 1), (4, 1),
        (3, 1), (2, 1), (5, 0), (4, 0), (1, 0), (0, 0), (1, 1), (0, 1),
    ]
    w_copies = {}
    for e, h in order:
        at = pl.ds(pl.multiple_of(flipped(me, e) * cols + h * half, half), half)
        w_copies[e, h] = pltpu.make_async_copy(w_hbm.at[:, at], weights.at[e, h], w_sems.at[e, h])
        w_copies[e, h].start()
    greet("tp", (sib, nx, ny))
    make, used = sender("tp", send_sems, recv_sems)
    to_sib = {
        (e, h): make(terms.at[e, h], from_sib.at[e // 2, h], sib) for e in (1, 3, 5, 7) for h in (0, 1)
    }
    six_x = make(sums.at[3, 0], from_six.at[0], nx)
    six_y = make(sums.at[3, 1], from_six.at[1], ny)
    to_x = [make(sums.at[1, h], from_x.at[h], nx) for h in (0, 1)]
    to_y = [make(sums.at[2, h], from_y.at[h], ny) for h in (0, 1)]

    def term(e, h):
        w_copies[e, h].wait()

        @pl.loop(0, half // 256)
        def _(t):
            at = pl.ds(pl.multiple_of(t * 256, 256), 256)
            terms[e, h, :, at] = jnp.dot(
                a_ref[...], weights[e, h, :, at], preferred_element_type=jnp.float32
            ).astype(jnp.bfloat16)

        if e % 2:
            to_sib[e, h].start()

    def summed(e, h, others, target):
        to_sib[e + 1, h].wait_recv()

        @pl.loop(0, rows // 64)
        def _(i):
            at = pl.ds(pl.multiple_of(i * 64, 64), 64)
            total = terms[e, h, at, :].astype(jnp.float32)
            total = total + from_sib[e // 2, h, at, :].astype(jnp.float32)
            for other in others:
                total = total + other[at, :].astype(jnp.float32)
            target[at, :] = total.astype(jnp.bfloat16)

    term(7, 0)
    term(6, 0)
    summed(6, 0, (), sums.at[3, 0])
    six_x.start()
    term(7, 1)
    term(6, 1)
    summed(6, 1, (), sums.at[3, 1])
    six_y.start()
    term(3, 0)
    term(2, 0)
    summed(2, 0, (), sums.at[1, 0])
    to_x[0].start()
    term(5, 1)
    term(4, 1)
    summed(4, 1, (), sums.at[2, 1])
    to_y[1].start()
    term(3, 1)
    term(2, 1)
    term(5, 0)
    term(4, 0)
    six_x.wait_recv()
    summed(4, 0, (from_six.at[0],), sums.at[2, 0])
    to_y[0].start()
    six_y.wait_recv()
    summed(2, 1, (from_six.at[1],), sums.at[1, 1])
    to_x[1].start()
    term(1, 0)
    term(0, 0)
    term(1, 1)
    term(0, 1)
    for h in (0, 1):
        to_x[h].wait_recv()
        to_y[h].wait_recv()
        summed(0, h, (from_x.at[h], from_y.at[h]), out_ref.at[:, pl.ds(h * half, half)])
    for copy in used:
        copy.wait_send()


def shards(
    n_cp, n_tp, checkpoint, norm_gain, query_weight, key_weight, value_weight, output_weight, block_order
):
    rows, depth = checkpoint.shape
    q_cols = query_weight.shape[1]
    k_cols = key_weight.shape[1]
    heads = q_cols // HEAD_DIM
    block = rows // 2
    context_rank = lax.axis_index("cp")
    own_blocks = lax.dynamic_slice_in_dim(block_order, 2 * context_rank, 2)
    offsets = jnp.arange(block, dtype=jnp.int32)
    positions = (own_blocks[:, None] * block + offsets[None, :]).reshape(rows)
    lanes = jnp.arange(HEAD_DIM, dtype=jnp.int32)
    rates = rope_base ** (-2.0 * (lanes // 2).astype(jnp.float32) / HEAD_DIM)
    angles = positions.astype(jnp.float32)[:, None] * rates[None, :]
    cosine = jnp.cos(angles)
    sine = jnp.where(lanes % 2 == 0, -1.0, 1.0)[None, :] * jnp.sin(angles)

    any_spec = pl.BlockSpec(memory_space=pl.ANY)
    vmem = pl.BlockSpec(memory_space=pltpu.VMEM)
    smem = pl.BlockSpec(memory_space=pltpu.SMEM)
    bf16, f32 = jnp.bfloat16, jnp.float32
    dma = pltpu.SemaphoreType.DMA

    if n_tp == 8:
        queries, key_value = pl.pallas_call(
            project_kernel,
            out_shape=(
                jax.ShapeDtypeStruct((rows, q_cols), bf16),
                jax.ShapeDtypeStruct((rows, 2 * k_cols), bf16),
            ),
            in_specs=[any_spec, vmem, any_spec, any_spec, any_spec, vmem, vmem],
            out_specs=(vmem, vmem),
            scratch_shapes=[
                pltpu.VMEM((8, rows, depth), bf16),
                pltpu.VMEM((8, depth, q_cols + 2 * k_cols), bf16),
                pltpu.VMEM((8, 1, depth), f32),
                pltpu.VMEM((rows, q_cols + 2 * k_cols), f32),
                pltpu.VMEM((rows, depth), bf16),
                pltpu.VMEM((rows, 1), f32),
                dma,
                dma((8, 3)),
                dma((13,)),
                dma((13,)),
            ],
            compiler_params=pltpu.CompilerParams(
                collective_id=0, has_side_effects=True, vmem_limit_bytes=VMEM_BYTES
            ),
            name="project",
        )(
            checkpoint, norm_gain.reshape(-1, depth), query_weight, key_weight, value_weight, cosine, sine
        )
    else:
        queries, key_value = project_any(
            checkpoint, norm_gain, query_weight, key_weight, value_weight, positions
        )

    attended, normalizer = pl.pallas_call(
        functools.partial(attend_kernel, n_cp),
        out_shape=(
            jax.ShapeDtypeStruct((rows, q_cols), bf16),
            jax.ShapeDtypeStruct((heads, rows), f32),
        ),
        in_specs=[smem, vmem, any_spec],
        out_specs=(vmem, vmem),
        scratch_shapes=[
            pltpu.VMEM((n_cp, rows, 2 * HEAD_DIM), bf16),
            pltpu.VMEM((rows, 2 * HEAD_DIM), bf16),
            pltpu.VMEM((rows, rows), f32),
            pltpu.VMEM((heads, rows, 1), f32),
            pltpu.VMEM((heads, rows, 2 * HEAD_DIM), f32),
            pltpu.VMEM((rows, HEAD_DIM), f32),
            dma,
            dma((n_cp - 1, 2)),
            dma((n_cp - 1, 2)),
        ],
        compiler_params=pltpu.CompilerParams(
            collective_id=1, has_side_effects=True, vmem_limit_bytes=VMEM_BYTES
        ),
        name="attend",
    )(block_order, queries, key_value)

    if n_tp != 8:
        partial_terms = jnp.dot(attended, output_weight, preferred_element_type=jnp.float32)
        projected = lax.psum_scatter(
            partial_terms.astype(bf16), "tp", scatter_dimension=1, tiled=True
        )
        return (projected, normalizer)

    out_cols = output_weight.shape[1] // n_tp
    half = out_cols // 2
    projected = pl.pallas_call(
        output_kernel,
        out_shape=jax.ShapeDtypeStruct((rows, out_cols), bf16),
        in_specs=[vmem, any_spec],
        out_specs=vmem,
        scratch_shapes=[
            pltpu.VMEM((8, 2, q_cols, half), bf16),
            pltpu.VMEM((8, 2, rows, half), bf16),
            pltpu.VMEM((4, 2, rows, half), bf16),
            pltpu.VMEM((4, 2, rows, half), bf16),
            pltpu.VMEM((2, rows, half), bf16),
            pltpu.VMEM((2, rows, half), bf16),
            pltpu.VMEM((2, rows, half), bf16),
            dma((8, 2)),
            dma((14,)),
            dma((14,)),
        ],
        compiler_params=pltpu.CompilerParams(
            collective_id=2, has_side_effects=True, vmem_limit_bytes=VMEM_BYTES
        ),
        name="project_out",
    )(attended, output_weight)
    return (projected, normalizer)


def solution(mesh):
    return jax.shard_map(
        functools.partial(shards, mesh.shape["cp"], mesh.shape["tp"]),
        mesh=mesh,
        in_specs=(
            P("cp", "tp"),
            P(),
            P(None, "tp"),
            P(None, "tp"),
            P(None, "tp"),
            P("tp", None),
            P(),
        ),
        out_specs=(P("cp", "tp"), P("tp", "cp")),
        check_vma=False,
    )
```

```python
import functools
import math

import jax
import jax.numpy as jnp
from jax import lax
from jax.experimental import pallas as pl
from jax.experimental.pallas import tpu as pltpu
from jax.sharding import PartitionSpec as P

HEAD_DIM = 128
KV_HEADS = 8
MESH = pl.DeviceIdType.MESH
VMEM_BYTES = 62 * 1024 * 1024

rope_base = 500000.0
norm_epsilon = 1e-05
masked_score = -1e30
LOG2E = 1.4426950408889634


def partner_2(block, axis, stride):
    count = lax.axis_size(axis)
    route = []
    for low in range(count):
        high = low | 1 << stride
        if high != low and high < count:
            route += [(low, high), (high, low)]
    return lax.ppermute(block, axis, route)


def turn_pairs(matrix, positions, first_pair):
    pair_count = matrix.shape[-1] // 2
    pair_index = (first_pair + jnp.arange(pair_count, dtype=jnp.int32)).astype(jnp.float32)
    inverse_rates = rope_base ** (-2.0 * pair_index / HEAD_DIM)
    angles = positions.astype(jnp.float32)[:, None] * inverse_rates[None, :]
    cosine = jnp.cos(angles)[:, None, :]
    sine_part = jnp.sin(angles)[:, None, :]
    paired = matrix.reshape(matrix.shape[0], matrix.shape[1], pair_count, 2)
    former = paired[..., 0]
    latter = paired[..., 1]
    turned = jnp.stack(
        [former * cosine - latter * sine_part, former * sine_part + latter * cosine], axis=-1
    )
    return turned.reshape(matrix.shape)


def project_any(checkpoint, norm_gain, query_weight, key_weight, value_weight, positions):
    rows = checkpoint.shape[0]
    heads = query_weight.shape[1] // HEAD_DIM
    key_columns = key_weight.shape[1]
    gathered = lax.all_gather(checkpoint, "tp", axis=1, tiled=True)
    widened = gathered.astype(jnp.float32)
    mean_square = jnp.mean(widened * widened, axis=-1, keepdims=True)
    normed = (widened * lax.rsqrt(mean_square + norm_epsilon) * norm_gain).astype(jnp.bfloat16)
    query_features = jnp.dot(normed, query_weight, preferred_element_type=jnp.float32)
    key_features = jnp.dot(normed, key_weight, preferred_element_type=jnp.float32)
    value_features = jnp.dot(normed, value_weight, preferred_element_type=jnp.float32)
    turned = turn_pairs(query_features.reshape(rows, heads, HEAD_DIM), positions, 0)
    queries = (turned * (LOG2E / math.sqrt(HEAD_DIM))).astype(jnp.bfloat16)
    sharing = lax.axis_size("tp") // KV_HEADS
    part_of_head = lax.axis_index("tp") % sharing
    key_part = turn_pairs(
        key_features.reshape(rows, 1, key_columns), positions, part_of_head * (key_columns // 2)
    )
    key_part = key_part.astype(jnp.bfloat16).reshape(rows, key_columns)
    own_pair = jnp.stack([key_part, value_features.astype(jnp.bfloat16)])
    key_value = own_pair
    if sharing == 2:
        partner = partner_2(own_pair, "tp", 0)
        lower_first = jnp.concatenate([own_pair, partner], axis=-1)
        upper_first = jnp.concatenate([partner, own_pair], axis=-1)
        key_value = jnp.where(part_of_head == 0, lower_first, upper_first)
    return (
        queries.reshape(rows, heads * HEAD_DIM),
        jnp.concatenate([key_value[0], key_value[1]], axis=-1),
    )


def flipped(me, offset):
    result = me
    for bit in (1, 2, 4):
        if offset & bit:
            result = result + bit - 2 * bit * lax.rem(lax.div(me, bit), 2)
    return result


def greet(axis, others):
    barrier = pltpu.get_barrier_semaphore()
    for other in others:
        pl.semaphore_signal(barrier, inc=1, device_id={axis: other}, device_id_type=MESH)
    pl.semaphore_wait(barrier, len(others))


def sender(axis, send_sems, recv_sems):
    used = []

    def make(source, target, other):
        index = len(used)
        copy = pltpu.make_async_remote_copy(
            src_ref=source,
            dst_ref=target,
            send_sem=send_sems.at[index],
            recv_sem=recv_sems.at[index],
            device_id={axis: other},
            device_id_type=MESH,
        )
        used.append(copy)
        return copy

    return make, used


def project_kernel(
    x_hbm, gain_ref, wq_hbm, wk_hbm, wv_hbm, cos_ref, sin_ref,
    q_ref, kv_ref,
    held, weights, gains, acc, scaled, squares, x_sem, w_sems, send_sems, recv_sems,
):
    me = lax.axis_index("tp")
    rows, depth = x_hbm.shape
    half = depth // 2
    q_cols = wq_hbm.shape[1]
    k_cols = wk_hbm.shape[1]
    sib, nx, ny = flipped(me, 1), flipped(me, 2), flipped(me, 4)
    x_copies = [
        pltpu.make_async_copy(x_hbm.at[:, pl.ds(h * half, half)], held.at[0, h], x_sem.at[h])
        for h in range(2)
    ]
    for copy in x_copies:
        copy.start()
    w_copies = []
    for e in range(8):
        chunk = pl.ds(pl.multiple_of(flipped(me, e) * depth, depth), depth)
        parts = (
            (wq_hbm, 0, q_cols),
            (wk_hbm, q_cols, k_cols),
            (wv_hbm, q_cols + k_cols, k_cols),
        )
        w_copies.append(
            [
                pltpu.make_async_copy(
                    w.at[chunk, :], weights.at[e, :, pl.ds(at, size)], w_sems.at[e, i]
                )
                for i, (w, at, size) in enumerate(parts)
            ]
        )
    for copies in w_copies:
        for copy in copies:
            copy.start()
    greet("tp", (sib, nx, ny))
    for copy in x_copies:
        copy.wait()
    make, used = sender("tp", send_sems, recv_sems)

    def part(slot, h):
        return held.at[slot, h]

    dx = [make(part(0, h), part(2, h), nx) for h in range(2)]
    dy = [make(part(0, h), part(4, h), ny) for h in range(2)]
    d1 = make(held.at[0], held.at[1], sib)
    forward_y = make(part(2, 0), part(6, 0), ny)
    forward_x = make(part(4, 1), part(6, 1), nx)
    d3 = [make(part(2, h), part(3, h), sib) for h in range(2)]
    d5 = [make(part(4, h), part(5, h), sib) for h in range(2)]
    d7 = [make(part(6, h), part(7, h), sib) for h in range(2)]
    dx[0].start()
    dy[1].start()
    dx[1].start()
    dy[0].start()
    d1.start()

    squares[...] = jnp.zeros_like(squares)
    acc[...] = jnp.zeros_like(acc)
    for e in range(8):
        at = pl.ds(pl.multiple_of(flipped(me, e) * depth, depth), depth)
        gains[e] = gain_ref[:, at]

    def process(e, h):
        @pl.loop(0, rows // 64)
        def _(i):
            at = pl.ds(pl.multiple_of(i * 64, 64), 64)
            wide = held[e, h, at, :].astype(jnp.float32)
            squares[at, :] += jnp.sum(wide * wide, axis=1, keepdims=True)
            gain = gains[e, :, h * half : (h + 1) * half]
            scaled[at, :] = (wide * gain).astype(jnp.bfloat16)

        @pl.loop(0, (q_cols + 2 * k_cols) // 256)
        def _(t):
            at = pl.ds(pl.multiple_of(t * 256, 256), 256)
            acc[:, at] += jnp.dot(
                scaled[...],
                weights[e, h * half : (h + 1) * half, at],
                preferred_element_type=jnp.float32,
            )

    def weights_of(*slots):
        for e in slots:
            for copy in w_copies[e]:
                copy.wait()

    weights_of(0)
    process(0, 0)
    process(0, 1)
    weights_of(1)
    d1.wait_recv()
    process(1, 0)
    process(1, 1)
    dx[0].wait_recv()
    forward_y.start()
    d3[0].start()
    dy[1].wait_recv()
    forward_x.start()
    d5[1].start()
    weights_of(2, 3, 4, 5)
    process(2, 0)
    process(4, 1)
    d3[0].wait_recv()
    process(3, 0)
    d5[1].wait_recv()
    process(5, 1)
    dx[1].wait_recv()
    d3[1].start()
    dy[0].wait_recv()
    d5[0].start()
    process(2, 1)
    process(4, 0)
    d3[1].wait_recv()
    process(3, 1)
    d5[0].wait_recv()
    process(5, 0)
    weights_of(6, 7)
    forward_y.wait_recv()
    d7[0].start()
    forward_x.wait_recv()
    d7[1].start()
    process(6, 0)
    process(6, 1)
    d7[0].wait_recv()
    process(7, 0)
    d7[1].wait_recv()
    process(7, 1)

    score_scale = LOG2E / math.sqrt(HEAD_DIM)
    features = depth * 8

    @pl.loop(0, rows // 64)
    def _(i):
        at = pl.ds(pl.multiple_of(i * 64, 64), 64)
        rate = lax.rsqrt(squares[at, :] * (1.0 / features) + norm_epsilon)
        cosine = cos_ref[at, :]
        sine = sin_ref[at, :]
        even = lax.rem(lax.broadcasted_iota(jnp.int32, (64, HEAD_DIM), 1), 2) == 0

        def turned(block):
            later = pltpu.roll(block, HEAD_DIM - 1, 1)
            former = pltpu.roll(block, 1, 1)
            return block * cosine + jnp.where(even, later, former) * sine

        for h in range(q_cols // HEAD_DIM):
            cols = pl.ds(h * HEAD_DIM, HEAD_DIM)
            q_ref[at, cols] = turned(acc[at, cols] * (rate * score_scale)).astype(jnp.bfloat16)
        keys = acc[at, pl.ds(q_cols, k_cols)] * rate
        kv_ref[at, pl.ds(0, k_cols)] = turned(keys).astype(jnp.bfloat16)
        values = acc[at, pl.ds(q_cols + k_cols, k_cols)] * rate
        kv_ref[at, pl.ds(k_cols, k_cols)] = values.astype(jnp.bfloat16)

    for copy in used:
        copy.wait_send()


def attend_kernel(
    n_cp, order_ref, q_ref, kv_hbm, out_ref, norm_ref,
    ring, extended, bias, top, weighted, norms, kv_sem, send_sems, recv_sems,
):
    me = lax.axis_index("cp")
    rows = q_ref.shape[0]
    block = rows // 2
    heads = q_ref.shape[1] // HEAD_DIM
    right, left = lax.rem(me + 1, n_cp), lax.rem(me + n_cp - 1, n_cp)
    own_copy = pltpu.make_async_copy(kv_hbm, ring.at[0], kv_sem)
    own_copy.start()
    greet("cp", (right, left))
    own_copy.wait()

    def hop(step, h):
        at = pl.ds(h * block, block)
        return pltpu.make_async_remote_copy(
            src_ref=ring.at[step, at, :],
            dst_ref=ring.at[step + 1, at, :],
            send_sem=send_sems.at[step, h],
            recv_sem=recv_sems.at[step, h],
            device_id={"cp": right},
            device_id_type=MESH,
        )

    hop(0, 0).start()
    hop(0, 1).start()
    extended[:, HEAD_DIM:] = jnp.ones((rows, HEAD_DIM), jnp.bfloat16)
    top[...] = jnp.full(top.shape, masked_score, jnp.float32)
    weighted[...] = jnp.zeros_like(weighted)

    def visit(step, carried):
        for h in range(2):

            @pl.when(step > 0)
            def _():
                hop(step - 1, h).wait_recv()

            @pl.when(jnp.logical_and(step > 0, step < n_cp - 1))
            def _():
                hop(step, h).start()

        owner = lax.rem(me - step + n_cp, n_cp)
        extended[:, :HEAD_DIM] = ring[step, :, HEAD_DIM:]
        base = lax.broadcasted_iota(jnp.int32, (block, block), 0) - lax.broadcasted_iota(
            jnp.int32, (block, block), 1
        )
        for i in range(2):
            for j in range(2):
                ahead = (order_ref[2 * me + i] - order_ref[2 * owner + j]) * block
                bias[i * block : (i + 1) * block, j * block : (j + 1) * block] = jnp.where(
                    base + ahead >= 0, 0.0, masked_score
                )

        def one_head(h, inner):
            cols = pl.ds(pl.multiple_of(h * HEAD_DIM, HEAD_DIM), HEAD_DIM)
            keys = ring[step, :, :HEAD_DIM]
            for i in range(2):
                at = pl.ds(i * block, block)
                scores = lax.dot_general(
                    q_ref[at, cols], keys, (((1,), (1,)), ((), ())),
                    preferred_element_type=jnp.float32,
                )
                scores = scores + bias[at, :]
                old_top = top[h, at, :]
                new_top = jnp.maximum(old_top, jnp.max(scores, axis=1, keepdims=True))
                weights = jnp.exp2(scores - new_top).astype(jnp.bfloat16)
                shrink = jnp.exp2(old_top - new_top)
                top[h, at, :] = new_top
                weighted[h, at, :] = weighted[h, at, :] * shrink + jnp.dot(
                    weights, extended[...], preferred_element_type=jnp.float32
                )
            return inner

        lax.fori_loop(0, heads, one_head, 0, unroll=2)
        return carried

    lax.fori_loop(0, n_cp, visit, 0)
    lane = lax.broadcasted_iota(jnp.int32, (rows, HEAD_DIM), 1)
    norms[...] = jnp.zeros_like(norms)
    for h in range(heads):
        totals = weighted[h, :, HEAD_DIM:]
        out_ref[:, h * HEAD_DIM : (h + 1) * HEAD_DIM] = (
            weighted[h, :, :HEAD_DIM] / totals
        ).astype(jnp.bfloat16)
        norm = (top[h] + jnp.log2(totals)) * (1.0 / LOG2E)
        norms[...] = jnp.where(lane == h, norm, norms[...])
    norm_ref[...] = jnp.transpose(norms[...])[:heads, :]

    for step in range(n_cp - 1):
        for h in range(2):
            hop(step, h).wait_send()


def output_kernel(
    a_ref, w_hbm, out_ref,
    weights, terms, sums, from_sib, from_six, from_x, from_y, w_sems, send_sems, recv_sems,
):
    me = lax.axis_index("tp")
    rows, depth = a_ref.shape
    cols = out_ref.shape[1]
    half = cols // 2
    sib, nx, ny = flipped(me, 1), flipped(me, 2), flipped(me, 4)
    order = [
        (7, 0), (6, 0), (7, 1), (6, 1), (3, 0), (2, 0), (5, 1), (4, 1),
        (3, 1), (2, 1), (5, 0), (4, 0), (1, 0), (0, 0), (1, 1), (0, 1),
    ]
    w_copies = {}
    for e, h in order:
        at = pl.ds(pl.multiple_of(flipped(me, e) * cols + h * half, half), half)
        w_copies[e, h] = pltpu.make_async_copy(w_hbm.at[:, at], weights.at[e, h], w_sems.at[e, h])
        w_copies[e, h].start()
    greet("tp", (sib, nx, ny))
    make, used = sender("tp", send_sems, recv_sems)
    to_sib = {
        (e, h): make(terms.at[e, h], from_sib.at[e // 2, h], sib) for e in (1, 3, 5, 7) for h in (0, 1)
    }
    six_x = make(sums.at[3, 0], from_six.at[0], nx)
    six_y = make(sums.at[3, 1], from_six.at[1], ny)
    to_x = [make(sums.at[1, h], from_x.at[h], nx) for h in (0, 1)]
    to_y = [make(sums.at[2, h], from_y.at[h], ny) for h in (0, 1)]

    def term(e, h):
        w_copies[e, h].wait()

        @pl.loop(0, half // 256)
        def _(t):
            at = pl.ds(pl.multiple_of(t * 256, 256), 256)
            terms[e, h, :, at] = jnp.dot(
                a_ref[...], weights[e, h, :, at], preferred_element_type=jnp.float32
            ).astype(jnp.bfloat16)

        if e % 2:
            to_sib[e, h].start()

    def summed(e, h, others, target):
        to_sib[e + 1, h].wait_recv()

        @pl.loop(0, rows // 64)
        def _(i):
            at = pl.ds(pl.multiple_of(i * 64, 64), 64)
            total = terms[e, h, at, :].astype(jnp.float32)
            total = total + from_sib[e // 2, h, at, :].astype(jnp.float32)
            for other in others:
                total = total + other[at, :].astype(jnp.float32)
            target[at, :] = total.astype(jnp.bfloat16)

    term(7, 0)
    term(6, 0)
    summed(6, 0, (), sums.at[3, 0])
    six_x.start()
    term(7, 1)
    term(6, 1)
    summed(6, 1, (), sums.at[3, 1])
    six_y.start()
    term(3, 0)
    term(2, 0)
    summed(2, 0, (), sums.at[1, 0])
    to_x[0].start()
    term(5, 1)
    term(4, 1)
    summed(4, 1, (), sums.at[2, 1])
    to_y[1].start()
    term(3, 1)
    term(2, 1)
    term(5, 0)
    term(4, 0)
    six_x.wait_recv()
    summed(4, 0, (from_six.at[0],), sums.at[2, 0])
    to_y[0].start()
    six_y.wait_recv()
    summed(2, 1, (from_six.at[1],), sums.at[1, 1])
    to_x[1].start()
    term(1, 0)
    term(0, 0)
    term(1, 1)
    term(0, 1)
    for h in (0, 1):
        to_x[h].wait_recv()
        to_y[h].wait_recv()
        summed(0, h, (from_x.at[h], from_y.at[h]), out_ref.at[:, pl.ds(h * half, half)])
    for copy in used:
        copy.wait_send()


def shards(
    n_cp, n_tp, checkpoint, norm_gain, query_weight, key_weight, value_weight, output_weight, block_order
):
    rows, depth = checkpoint.shape
    q_cols = query_weight.shape[1]
    k_cols = key_weight.shape[1]
    heads = q_cols // HEAD_DIM
    block = rows // 2
    context_rank = lax.axis_index("cp")
    own_blocks = lax.dynamic_slice_in_dim(block_order, 2 * context_rank, 2)
    offsets = jnp.arange(block, dtype=jnp.int32)
    positions = (own_blocks[:, None] * block + offsets[None, :]).reshape(rows)
    lanes = jnp.arange(HEAD_DIM, dtype=jnp.int32)
    rates = rope_base ** (-2.0 * (lanes // 2).astype(jnp.float32) / HEAD_DIM)
    angles = positions.astype(jnp.float32)[:, None] * rates[None, :]
    cosine = jnp.cos(angles)
    sine = jnp.where(lanes % 2 == 0, -1.0, 1.0)[None, :] * jnp.sin(angles)

    any_spec = pl.BlockSpec(memory_space=pl.ANY)
    vmem = pl.BlockSpec(memory_space=pltpu.VMEM)
    smem = pl.BlockSpec(memory_space=pltpu.SMEM)
    bf16, f32 = jnp.bfloat16, jnp.float32
    dma = pltpu.SemaphoreType.DMA

    if n_tp == 8:
        queries, key_value = pl.pallas_call(
            project_kernel,
            out_shape=(
                jax.ShapeDtypeStruct((rows, q_cols), bf16),
                jax.ShapeDtypeStruct((rows, 2 * k_cols), bf16),
            ),
            in_specs=[any_spec, vmem, any_spec, any_spec, any_spec, vmem, vmem],
            out_specs=(vmem, vmem),
            scratch_shapes=[
                pltpu.VMEM((8, 2, rows, depth // 2), bf16),
                pltpu.VMEM((8, depth, q_cols + 2 * k_cols), bf16),
                pltpu.VMEM((8, 1, depth), f32),
                pltpu.VMEM((rows, q_cols + 2 * k_cols), f32),
                pltpu.VMEM((rows, depth // 2), bf16),
                pltpu.VMEM((rows, 1), f32),
                dma((2,)),
                dma((8, 3)),
                dma((13,)),
                dma((13,)),
            ],
            compiler_params=pltpu.CompilerParams(
                collective_id=0, has_side_effects=True, vmem_limit_bytes=VMEM_BYTES
            ),
            name="project",
        )(
            checkpoint, norm_gain.reshape(1, -1), query_weight, key_weight, value_weight, cosine, sine
        )
    else:
        queries, key_value = project_any(
            checkpoint, norm_gain, query_weight, key_weight, value_weight, positions
        )

    attended, normalizer = pl.pallas_call(
        functools.partial(attend_kernel, n_cp),
        out_shape=(
            jax.ShapeDtypeStruct((rows, q_cols), bf16),
            jax.ShapeDtypeStruct((heads, rows), f32),
        ),
        in_specs=[smem, vmem, any_spec],
        out_specs=(vmem, vmem),
        scratch_shapes=[
            pltpu.VMEM((n_cp, rows, 2 * HEAD_DIM), bf16),
            pltpu.VMEM((rows, 2 * HEAD_DIM), bf16),
            pltpu.VMEM((rows, rows), f32),
            pltpu.VMEM((heads, rows, 1), f32),
            pltpu.VMEM((heads, rows, 2 * HEAD_DIM), f32),
            pltpu.VMEM((rows, HEAD_DIM), f32),
            dma,
            dma((n_cp - 1, 2)),
            dma((n_cp - 1, 2)),
        ],
        compiler_params=pltpu.CompilerParams(
            collective_id=1, has_side_effects=True, vmem_limit_bytes=VMEM_BYTES
        ),
        name="attend",
    )(block_order, queries, key_value)

    if n_tp != 8:
        partial_terms = jnp.dot(attended, output_weight, preferred_element_type=jnp.float32)
        projected = lax.psum_scatter(
            partial_terms.astype(bf16), "tp", scatter_dimension=1, tiled=True
        )
        return (projected, normalizer)

    out_cols = output_weight.shape[1] // n_tp
    half = out_cols // 2
    projected = pl.pallas_call(
        output_kernel,
        out_shape=jax.ShapeDtypeStruct((rows, out_cols), bf16),
        in_specs=[vmem, any_spec],
        out_specs=vmem,
        scratch_shapes=[
            pltpu.VMEM((8, 2, q_cols, half), bf16),
            pltpu.VMEM((8, 2, rows, half), bf16),
            pltpu.VMEM((4, 2, rows, half), bf16),
            pltpu.VMEM((4, 2, rows, half), bf16),
            pltpu.VMEM((2, rows, half), bf16),
            pltpu.VMEM((2, rows, half), bf16),
            pltpu.VMEM((2, rows, half), bf16),
            dma((8, 2)),
            dma((14,)),
            dma((14,)),
        ],
        compiler_params=pltpu.CompilerParams(
            collective_id=2, has_side_effects=True, vmem_limit_bytes=VMEM_BYTES
        ),
        name="project_out",
    )(attended, output_weight)
    return (projected, normalizer)


def solution(mesh):
    return jax.shard_map(
        functools.partial(shards, mesh.shape["cp"], mesh.shape["tp"]),
        mesh=mesh,
        in_specs=(
            P("cp", "tp"),
            P(),
            P(None, "tp"),
            P(None, "tp"),
            P(None, "tp"),
            P("tp", None),
            P(),
        ),
        out_specs=(P("cp", "tp"), P("tp", "cp")),
        check_vma=False,
    )
```
